32 devices in a mesh: dp: 2 (over x), tp: 4 (over z), cp: 4 (over y, core).
Axes of the slice: x: 2, y: 2, z: 4, core: 2. Of those that a mesh axis runs over, the one named last changes fastest.
Arguments:
- x_in: bfloat16 [16384, 4096], P(('dp', 'cp', 'tp')), parts along dimension 0
- seg_ids: int32 [16384], P(('dp', 'cp', 'tp')), parts along dimension 0
- w_q: bfloat16 [4096, 32, 128], P(None, 'tp')
- w_k: bfloat16 [4096, 8, 128], P(None, 'tp')
- w_v: bfloat16 [4096, 8, 128], P(None, 'tp')
- w_o: bfloat16 [32, 128, 4096], P('tp')
Outputs:
- output: bfloat16 [16384, 4096], P(('dp', 'cp', 'tp')), parts along dimension 0
There are 2 independent parts. The reference program is written for one: setup_inputs(seed, part) draws one part's arguments, and reference() takes and returns one part's arrays. A program takes and returns all parts, laid end to end along the dimension named above; an argument that names none is the same for every part.
All inputs are finite; a program needn't handle non-finite values.
Results may differ from the reference program's by a relative error of at most 0.00421059.
Values are sent between devices in bfloat16 or wider.
A program may use at most 1 GiB of HBM per device.

```python
import jax
import jax.numpy as jnp
from jax import lax

CP = 4
PIECE = 1024
D = 4096
HEADS = 32
KV_HEADS = 8
HEAD = 128
DOCS = 6
QROWS = 64
SEQ = 2 * CP * PIECE
GROUP = HEADS // KV_HEADS


def row_positions():
    row_idx = jnp.arange(SEQ)
    owner_rank = row_idx // (2 * PIECE)
    within = row_idx % (2 * PIECE)
    return jnp.where(within < PIECE, owner_rank * PIECE + within, (2 * CP - 1 - owner_rank) * PIECE + within - PIECE)


def draw_segments(seg_key):
    half_len = SEQ // 2
    key_cut, key_gap = jax.random.split(seg_key)
    offsets = jax.random.permutation(key_cut, half_len - 1)[: DOCS - 1] + 1
    gap_start = jax.random.randint(key_gap, (), 0, half_len)
    cut_points = offsets + half_len * (offsets > gap_start).astype(jnp.int32)
    seq_pos = jnp.arange(SEQ)
    seg_seq = jnp.sum((seq_pos[:, None] >= cut_points[None, :]).astype(jnp.int32), axis=1)
    return seg_seq[row_positions()].astype(jnp.int32)


def setup_inputs(seed: int = 0, part: int = 0) -> dict:
    part_key = jax.random.fold_in(jax.random.key(seed), part)
    key_x, key_seg = jax.random.split(part_key)
    key_q, key_k, key_v, key_o = jax.random.split(jax.random.key(seed + 1), 4)
    x_in = jax.random.normal(key_x, (SEQ, D), jnp.float32).astype(jnp.bfloat16)
    seg_ids = draw_segments(key_seg)
    w_q = (jax.random.normal(key_q, (D, HEADS, HEAD), jnp.float32) * (1.5 * D ** -0.5)).astype(jnp.bfloat16)
    w_k = (jax.random.normal(key_k, (D, KV_HEADS, HEAD), jnp.float32) * D ** -0.5).astype(jnp.bfloat16)
    w_v = (jax.random.normal(key_v, (D, KV_HEADS, HEAD), jnp.float32) * D ** -0.5).astype(jnp.bfloat16)
    w_o = (jax.random.normal(key_o, (HEADS, HEAD, D), jnp.float32) * (4.0 * (HEADS * HEAD) ** -0.5)).astype(jnp.bfloat16)
    return {"x_in": x_in, "seg_ids": seg_ids, "w_q": w_q, "w_k": w_k, "w_v": w_v, "w_o": w_o}


def reference(x_in, seg_ids, w_q, w_k, w_v, w_o):
    pos_rows = row_positions()
    q_rows = jnp.dot(x_in, w_q.reshape(D, HEADS * HEAD), preferred_element_type=jnp.float32).astype(jnp.bfloat16)
    k_rows = jnp.dot(x_in, w_k.reshape(D, KV_HEADS * HEAD), preferred_element_type=jnp.float32).astype(jnp.bfloat16)
    v_rows = jnp.dot(x_in, w_v.reshape(D, KV_HEADS * HEAD), preferred_element_type=jnp.float32).astype(jnp.bfloat16)
    q_blocks = q_rows.reshape(SEQ // QROWS, QROWS, KV_HEADS, GROUP, HEAD).astype(jnp.float32)
    k_heads = k_rows.reshape(SEQ, KV_HEADS, HEAD).transpose(1, 0, 2).astype(jnp.float32)
    v_heads = v_rows.reshape(SEQ, KV_HEADS, HEAD).transpose(1, 0, 2).astype(jnp.float32)
    pos_blocks = pos_rows.reshape(SEQ // QROWS, QROWS)
    seg_blocks = seg_ids.reshape(SEQ // QROWS, QROWS)

    def query_block(blk_args):
        q_blk, pos_blk, seg_blk = blk_args
        visible = (seg_blk[:, None] == seg_ids[None, :]) & (pos_rows[None, :] <= pos_blk[:, None])

        def kv_head(head_args):
            q_head, k_head, v_head = head_args
            scores = jnp.einsum("qge,se->gqs", q_head, k_head) * HEAD ** -0.5
            scores = jnp.where(visible[None], scores, -jnp.inf)
            prob_rows = jnp.exp(scores - jnp.max(scores, axis=-1, keepdims=True))
            row_sum = jnp.sum(prob_rows, axis=-1)
            pv_sum = jnp.einsum("gqs,se->gqe", prob_rows.astype(jnp.bfloat16).astype(jnp.float32), v_head)
            return (pv_sum / row_sum[..., None]).astype(jnp.bfloat16)

        return lax.map(kv_head, (q_blk.transpose(1, 0, 2, 3), k_heads, v_heads))

    attn_rows = lax.map(query_block, (q_blocks, pos_blocks, seg_blocks))
    attn_rows = attn_rows.transpose(0, 3, 1, 2, 4).reshape(SEQ, HEADS * HEAD)
    y_out = jnp.dot(attn_rows, w_o.reshape(HEADS * HEAD, D), preferred_element_type=jnp.float32)
    return y_out.astype(jnp.bfloat16)
```

```python
import functools
import math

import jax
import jax.numpy as jnp
from jax import lax
from jax.experimental import pallas as pl
from jax.experimental.pallas import tpu as pltpu
from jax.sharding import PartitionSpec as P


NEG_BIG = -1e30
K_TILE = 512
HALVES = 2


def flash_kernel(n_cp, n_tp, group, exp_scale, bounds_ref, q_ref, *refs):
    k_refs, v_refs = refs[:HALVES], refs[HALVES:2 * HALVES]
    start_ref, o_ref, q_all, m_ref, l_ref, acc_ref = refs[2 * HALVES:]
    tile = pl.program_id(0)
    head_dim = q_all.shape[1]
    rows = q_ref.shape[0]
    per_piece = n_tp // 2
    sub = K_TILE // HALVES
    for head in range(group):
        q_all[pl.ds(head * rows, rows), :] = q_ref[:, head * head_dim:(head + 1) * head_dim]
    m_ref[...] = jnp.full_like(m_ref, NEG_BIG)
    l_ref[...] = jnp.zeros_like(l_ref)
    acc_ref[...] = jnp.zeros_like(acc_ref)
    first_pos = bounds_ref[0, tile]
    cp_rank = bounds_ref[5, 0]

    def step(masked, blk, carry):
        piece = blk // per_piece
        early = piece < n_cp
        owner = jnp.where(early, piece, 2 * n_cp - 1 - piece)
        slot = jnp.bitwise_xor(owner, cp_rank)
        part = blk % per_piece + jnp.where(early, 0, per_piece)
        off = pl.multiple_of((slot * n_tp + part) * sub, sub)
        k_blk = jnp.concatenate([ref[pl.ds(off, sub), :] for ref in k_refs], axis=0)
        v_blk = jnp.concatenate([ref[pl.ds(off, sub), :] for ref in v_refs], axis=0)
        scores = lax.dot_general(q_all[...], k_blk, (((1,), (1,)), ((), ())), preferred_element_type=jnp.float32) * exp_scale
        if masked:
            key_pos = blk * K_TILE + lax.broadcasted_iota(jnp.int32, (rows, K_TILE), 1)
            row_pos = first_pos + lax.broadcasted_iota(jnp.int32, (rows, K_TILE), 0)
            allowed = (key_pos >= start_ref[...]) & (key_pos <= row_pos)
            scores = jnp.where(allowed[None], scores.reshape(group, rows, K_TILE), NEG_BIG).reshape(group * rows, K_TILE)
        m_old = m_ref[...]
        m_new = jnp.maximum(m_old, jnp.max(scores, axis=1, keepdims=True))
        probs = [jnp.exp2(scores[:, j:j + head_dim] - m_new) for j in range(0, K_TILE, head_dim)]
        rescale = jnp.exp2(m_old - m_new)
        l_ref[...] = rescale * l_ref[...] + functools.reduce(jnp.add, probs)
        prob_blk = jnp.concatenate([prob.astype(jnp.bfloat16) for prob in probs], axis=1)
        acc_ref[...] = rescale * acc_ref[...] + jnp.dot(prob_blk, v_blk, preferred_element_type=jnp.float32)
        m_ref[...] = m_new
        return carry

    lo = bounds_ref[1, tile]
    mid = bounds_ref[2, tile]
    full_end = bounds_ref[3, tile]
    hi = bounds_ref[4, tile]
    lax.fori_loop(lo, mid, functools.partial(step, True), 0)
    lax.fori_loop(mid, full_end, functools.partial(step, False), 0)
    lax.fori_loop(full_end, hi, functools.partial(step, True), 0)
    out = acc_ref[...] / jnp.sum(l_ref[...], axis=1, keepdims=True)
    for head in range(group):
        o_ref[:, head * head_dim:(head + 1) * head_dim] = out[head * rows:(head + 1) * rows].astype(o_ref.dtype)


def flash(n_cp, n_tp, q_rows, kv_halves, kv_idx, kv_loc, head_dim, bounds, row_start):
    n_rows = q_rows.shape[0]
    tile = n_rows // n_tp
    group = q_rows.shape[1] // (kv_loc * head_dim)
    exp_scale = head_dim ** -0.5 * math.log2(math.e)
    stacked = group * tile
    n_keys = kv_halves[0].shape[0]
    grid_spec = pltpu.PrefetchScalarGridSpec(
        num_scalar_prefetch=1,
        grid=(n_tp,),
        in_specs=[pl.BlockSpec((tile, group * head_dim), lambda i, b: (i, kv_idx))]
        + [pl.BlockSpec((n_keys, head_dim), lambda i, b: (0, kv_idx))] * HALVES
        + [pl.BlockSpec((n_keys, head_dim), lambda i, b: (0, kv_loc + kv_idx))] * HALVES
        + [pl.BlockSpec((tile, 1), lambda i, b: (i, 0))],
        out_specs=pl.BlockSpec((tile, group * head_dim), lambda i, b: (i, 0)),
        scratch_shapes=[
            pltpu.VMEM((stacked, head_dim), jnp.bfloat16),
            pltpu.VMEM((stacked, head_dim), jnp.float32),
            pltpu.VMEM((stacked, head_dim), jnp.float32),
            pltpu.VMEM((stacked, head_dim), jnp.float32),
        ],
    )
    n_scores = n_rows * n_keys * HALVES // 4 * group
    return pl.pallas_call(
        functools.partial(flash_kernel, n_cp, n_tp, group, exp_scale),
        grid_spec=grid_spec,
        out_shape=jax.ShapeDtypeStruct((n_rows, group * head_dim), jnp.bfloat16),
        compiler_params=pltpu.CompilerParams(dimension_semantics=("arbitrary",), vmem_limit_bytes=48 << 20),
        cost_estimate=pl.CostEstimate(flops=4 * n_scores * head_dim, bytes_accessed=12 << 20, transcendentals=n_scores),
    )(bounds, q_rows, *kv_halves, *kv_halves, row_start)


def project_kernel(n_tp, heads, n_o, n_w, rank_ref, *refs):
    o_refs, w_refs = refs[:n_o], refs[n_o:n_o + n_w]
    y_ref, o_full = refs[-2:]
    n_cols = y_ref.shape[-1]
    head_dim = w_refs[0].shape[1]
    sub = o_refs[0].shape[0]
    n_kv = n_o // (HALVES * n_tp)

    @pl.when(pl.program_id(0) == 0)
    def _():
        for half in range(HALVES):
            for kv_idx in range(n_kv):
                for bit in range(n_tp):
                    piece = o_refs[(half * n_kv + kv_idx) * n_tp + bit]
                    source = jnp.bitwise_xor(rank_ref[0], bit)
                    for head in range(heads):
                        part = jnp.bitwise_xor(rank_ref[1], kv_idx * heads + head)
                        col = pl.multiple_of((part * n_tp + source) * head_dim, head_dim)
                        o_full[half * sub:(half + 1) * sub, pl.ds(col, head_dim)] = piece[:, head * head_dim:(head + 1) * head_dim]

    total = None
    start = 0
    for w_ref in w_refs:
        depth = w_ref.shape[0] * head_dim
        term = jnp.dot(o_full[:, start:start + depth], w_ref[...].reshape(depth, n_cols), preferred_element_type=jnp.float32)
        total = term if total is None else total + term
        start += depth
    y_ref[...] = total.astype(y_ref.dtype)


def project(ranks, n_tp, pieces, w_parts, heads, d_model, y_left=None, n_cols=512):
    head_dim, cols = w_parts[0].shape[1:]
    sub, piece_cols = pieces[0].shape
    rows = HALVES * sub
    depth = sum(part.shape[0] for part in w_parts) * head_dim
    first = 0 if y_left is None else cols // n_cols
    extra = [] if y_left is None else [y_left]
    grid_spec = pltpu.PrefetchScalarGridSpec(
        num_scalar_prefetch=1,
        grid=(cols // n_cols,),
        in_specs=[pl.BlockSpec((sub, piece_cols), lambda i, t: (0, 0))] * len(pieces)
        + [pl.BlockSpec((part.shape[0], head_dim, n_cols), lambda i, t: (0, 0, i)) for part in w_parts]
        + [pl.BlockSpec(memory_space=pl.ANY)] * len(extra),
        out_specs=pl.BlockSpec((rows, n_cols), lambda i, t: (0, first + i)),
        scratch_shapes=[pltpu.VMEM((rows, depth), jnp.bfloat16)],
    )
    return pl.pallas_call(
        functools.partial(project_kernel, n_tp, heads, len(pieces), len(w_parts)),
        grid_spec=grid_spec,
        out_shape=jax.ShapeDtypeStruct((rows, d_model), jnp.bfloat16),
        input_output_aliases={1 + len(pieces) + len(w_parts): 0} if extra else {},
        compiler_params=pltpu.CompilerParams(dimension_semantics=("arbitrary",), vmem_limit_bytes=48 << 20),
        cost_estimate=pl.CostEstimate(flops=2 * rows * depth * cols, bytes_accessed=24 << 20, transcendentals=0),
    )(ranks, *pieces, *w_parts, *extra)


def solution(mesh):
    n_cp = mesh.shape["cp"]
    n_tp = mesh.shape["tp"]
    n_dp = mesh.shape["dp"]

    def swap(arr, axis, bit):
        return lax.ppermute(arr, axis, [(src, src ^ bit) for src in range(mesh.shape[axis])])

    def per_device(x_loc, seg_loc, w_q, w_k, w_v, w_o):
        cp_rank = lax.axis_index("cp")
        tp_rank = lax.axis_index("tp")
        own_rows, d_model = x_loc.shape
        kv_loc = w_k.shape[1]
        head_dim = w_k.shape[2]
        n_rows = own_rows * n_tp
        piece_len = n_rows // 2
        width = w_q.shape[1] * head_dim
        sub = own_rows // HALVES

        part_rows = w_o.shape[0] * head_dim // (n_dp * n_cp)
        part_idx = lax.axis_index("dp") * n_cp + cp_rank
        w_o_part = lax.dynamic_slice_in_dim(w_o.reshape(width, d_model), part_idx * part_rows, part_rows)
        half_cols = d_model // 2
        mid_tp = n_tp // 2

        def gather_wo(side):
            w_tp = lax.all_gather(w_o_part[:, side * half_cols:(side + 1) * half_cols], "tp", axis=0)
            w_dp = swap(w_tp, "dp", 1)
            w_cp = swap(w_tp, "cp", 2)
            w_diag0 = swap(w_dp[:mid_tp], "cp", 2)
            w_diag1 = swap(w_cp[mid_tp:], "dp", 1)
            near = [w_tp, w_cp, w_dp, w_diag0, w_diag1]
            far = []
            for part in near:
                far.append(swap(part, "cp", 1))
            return [near[0], far[0], near[1], far[1], near[2], far[2], near[3], near[4], far[3], far[4]]

        x_halves = []
        for half in range(HALVES):
            x_halves.append(lax.all_gather(x_loc[half * sub:(half + 1) * sub], "tp", axis=0, tiled=True))
        w_sides = [gather_wo(side) for side in range(2)]
        seg_all = lax.all_gather(seg_loc, ("cp", "tp"), axis=0, tiled=True)
        w_q2 = w_q.reshape(d_model, width)
        w_kv = jnp.concatenate([w_k.reshape(d_model, -1), w_v.reshape(d_model, -1)], axis=1)

        seg_rows = lax.dynamic_slice_in_dim(seg_all, cp_rank * n_rows, n_rows)
        row_start = jnp.sum((seg_all[None, :] < seg_rows[:, None]).astype(jnp.int32), axis=1)
        tiles = n_rows // sub
        tile_row = jnp.arange(tiles) * sub
        first_pos = jnp.where(tile_row < piece_len, cp_rank * piece_len + tile_row, (2 * n_cp - 1 - cp_rank) * piece_len + tile_row - piece_len)
        start_tiles = row_start.reshape(tiles, sub)
        lo = start_tiles[:, 0] // K_TILE
        full_end = (first_pos + 1) // K_TILE
        mid = jnp.minimum(jnp.maximum((start_tiles[:, -1] + K_TILE - 1) // K_TILE, lo), full_end)
        hi = (first_pos + sub - 1) // K_TILE + 1
        bounds = jnp.stack([first_pos, lo, mid, full_end, hi, jnp.full_like(lo, cp_rank)]).astype(jnp.int32)
        bounds = bounds.reshape(-1, n_tp, HALVES)
        row_start = row_start.reshape(n_tp, HALVES, sub)
        x_halves[0], w_q2, w_kv, bounds, row_start = lax.optimization_barrier((x_halves[0], w_q2, w_kv, bounds, row_start))

        q_halves, kv_halves = [], []
        for x_half in x_halves:
            kv_own = jnp.dot(x_half, w_kv, preferred_element_type=jnp.float32).astype(jnp.bfloat16)
            kv_far = swap(kv_own, "cp", 2)
            kv_chip = swap(kv_own, "cp", 1)
            kv_diag = swap(kv_far, "cp", 1)
            kv_halves.append(jnp.concatenate([kv_own, kv_chip, kv_far, kv_diag], axis=0))
            q_halves.append(jnp.dot(x_half, w_q2, preferred_element_type=jnp.float32).astype(jnp.bfloat16))

        pieces = []
        for half in range(HALVES):
            for kv_idx in range(kv_loc):
                o_rows = flash(n_cp, n_tp, q_halves[half], kv_halves, kv_idx, kv_loc, head_dim, bounds[:, :, half], row_start[:, half].reshape(-1, 1))
                o_tiles = o_rows.reshape(n_tp, sub, -1)
                for bit in range(n_tp):
                    mine = lax.dynamic_index_in_dim(o_tiles, tp_rank ^ bit, 0, False)
                    pieces.append(swap(mine, "tp", bit) if bit else mine)
        ranks = jnp.stack([tp_rank, part_idx]).astype(jnp.int32)
        y_left = project(ranks, n_tp, pieces, w_sides[0], w_q.shape[1] // kv_loc, d_model)
        return project(ranks, n_tp, pieces, w_sides[1], w_q.shape[1] // kv_loc, d_model, y_left)


    return jax.shard_map(
        per_device,
        mesh=mesh,
        in_specs=(P(("dp", "cp", "tp"), None), P(("dp", "cp", "tp")), P(None, "tp", None), P(None, "tp", None), P(None, "tp", None), P("tp", None, None)),
        out_specs=P(("dp", "cp", "tp"), None),
        check_vma=False,
    )
```

```python
import functools
import math

import jax
import jax.numpy as jnp
from jax import lax
from jax.experimental import pallas as pl
from jax.experimental.pallas import tpu as pltpu
from jax.sharding import PartitionSpec as P


NEG_BIG = -1e30
SUBS = 2


def flash_kernel(n_cp, n_tp, group, n_parts, first_bit, exp_scale, bounds_ref, *refs):
    q_refs, k_refs, v_refs = refs[:n_parts], refs[n_parts:2 * n_parts], refs[2 * n_parts:3 * n_parts]
    start_ref = refs[3 * n_parts]
    o_refs = refs[3 * n_parts + 1:-4]
    q_all, m_ref, l_ref, acc_ref = refs[-4:]
    step_idx = pl.program_id(0)
    dest, sub = step_idx // SUBS, step_idx % SUBS
    tile = jnp.bitwise_xor(bounds_ref[6, 0], first_bit - dest) * SUBS + sub
    head_dim = q_all.shape[1]
    rows = start_ref.shape[0]
    per_piece = n_tp // 2
    for sub_idx in range(SUBS):
        @pl.when(sub == sub_idx)
        def _():
            begin = 0
            for ref in q_refs:
                first = max(begin, sub_idx * rows)
                last = min(begin + ref.shape[0], (sub_idx + 1) * rows)
                if first < last:
                    for head in range(group):
                        at = head * rows + first - sub_idx * rows
                        q_all[at:at + last - first, :] = ref[first - begin:last - begin, head * head_dim:(head + 1) * head_dim]
                begin += ref.shape[0]
    m_ref[...] = jnp.full_like(m_ref, NEG_BIG)
    l_ref[...] = jnp.zeros_like(l_ref)
    acc_ref[...] = jnp.zeros_like(acc_ref)
    first_pos = bounds_ref[0, tile]
    lo = bounds_ref[1, tile]
    mid = bounds_ref[2, tile]
    full_end = bounds_ref[3, tile]
    hi = bounds_ref[4, tile]
    cp_rank = bounds_ref[5, 0]

    def block(masked, blk):
        piece = blk // per_piece
        early = piece < n_cp
        owner = jnp.where(early, piece, 2 * n_cp - 1 - piece)
        slot = jnp.bitwise_xor(owner, cp_rank)
        chunk = slot * n_tp + blk % per_piece + jnp.where(early, 0, per_piece)

        def rows_of(part_refs):
            sizes = [ref.shape[0] // (n_cp * n_tp) for ref in part_refs]
            return jnp.concatenate([ref[pl.ds(pl.multiple_of(chunk * size, size), size), :] for ref, size in zip(part_refs, sizes)], axis=0)

        k_blk = rows_of(k_refs)
        v_blk = rows_of(v_refs)
        width = k_blk.shape[0]
        scores = lax.dot_general(q_all[...], k_blk, (((1,), (1,)), ((), ())), preferred_element_type=jnp.float32) * exp_scale
        if masked:
            key_pos = blk * width + lax.broadcasted_iota(jnp.int32, (rows, width), 1)
            row_pos = first_pos + lax.broadcasted_iota(jnp.int32, (rows, width), 0)
            allowed = (key_pos >= start_ref[...]) & (key_pos <= row_pos)
            scores = jnp.where(allowed[None], scores.reshape(group, rows, width), NEG_BIG).reshape(group * rows, width)
        m_old = m_ref[...]
        m_new = jnp.maximum(m_old, jnp.max(scores, axis=1, keepdims=True))
        probs = [jnp.exp2(scores[:, j:j + head_dim] - m_new) for j in range(0, width, head_dim)]
        rescale = jnp.exp2(m_old - m_new)
        l_ref[...] = rescale * l_ref[...] + functools.reduce(jnp.add, probs)
        prob_blk = jnp.concatenate([prob.astype(jnp.bfloat16) for prob in probs], axis=1)
        acc_ref[...] = rescale * acc_ref[...] + jnp.dot(prob_blk, v_blk, preferred_element_type=jnp.float32)
        m_ref[...] = m_new

    def step(blk, carry):
        full = (blk >= mid) & (blk < full_end)
        pl.when(full)(functools.partial(block, False, blk))
        pl.when(jnp.logical_not(full))(functools.partial(block, True, blk))
        return carry

    lax.fori_loop(lo, hi, step, 0)
    out = (acc_ref[...] / jnp.sum(l_ref[...], axis=1, keepdims=True)).astype(jnp.bfloat16)
    for idx, o_ref in enumerate(o_refs):
        @pl.when(dest == idx)
        def _():
            at = pl.multiple_of(sub * rows, rows)
            for head in range(group):
                o_ref[pl.ds(at, rows), head * head_dim:(head + 1) * head_dim] = out[head * rows:(head + 1) * rows]


def flash(n_cp, n_tp, first_bit, q_parts, kv_parts, head_dim, bounds, row_start):
    sizes = [q_part.shape[0] // n_tp for q_part in q_parts]
    tile = sum(sizes)
    cols = q_parts[0].shape[1]
    group = cols // head_dim
    exp_scale = head_dim ** -0.5 * math.log2(math.e)
    rows = tile // SUBS
    stacked = group * rows
    n_keys = [part.shape[0] for part in kv_parts]
    n_parts = len(sizes)
    grid_spec = pltpu.PrefetchScalarGridSpec(
        num_scalar_prefetch=1,
        grid=(2 * SUBS,),
        in_specs=[pl.BlockSpec((size, cols), lambda i, b: (jnp.bitwise_xor(b[6, 0], first_bit - i // SUBS), 0)) for size in sizes]
        + [pl.BlockSpec((keys, head_dim), lambda i, b: (0, 0)) for keys in n_keys]
        + [pl.BlockSpec((keys, head_dim), lambda i, b: (0, 1)) for keys in n_keys]
        + [pl.BlockSpec((rows, 1), lambda i, b: (jnp.bitwise_xor(b[6, 0], first_bit - i // SUBS) * SUBS + i % SUBS, 0))],
        out_specs=[pl.BlockSpec((tile, cols), lambda i, b: (0, 0))] * 2,
        scratch_shapes=[
            pltpu.VMEM((stacked, head_dim), jnp.bfloat16),
            pltpu.VMEM((stacked, head_dim), jnp.float32),
            pltpu.VMEM((stacked, head_dim), jnp.float32),
            pltpu.VMEM((stacked, head_dim), jnp.float32),
        ],
    )
    n_scores = stacked * SUBS * sum(n_keys)
    return pl.pallas_call(
        functools.partial(flash_kernel, n_cp, n_tp, group, n_parts, first_bit, exp_scale),
        grid_spec=grid_spec,
        out_shape=[jax.ShapeDtypeStruct((tile, cols), jnp.bfloat16)] * 2,
        compiler_params=pltpu.CompilerParams(dimension_semantics=("arbitrary",), vmem_limit_bytes=56 << 20),
        cost_estimate=pl.CostEstimate(flops=4 * n_scores * head_dim, bytes_accessed=12 << 20, transcendentals=n_scores),
    )(bounds, *q_parts, *kv_parts, *kv_parts, row_start)


def project_kernel(n_tp, heads, n_o, n_w, n_left, rank_ref, *refs):
    o_refs, sides = refs[:n_o], (refs[n_o:n_o + n_w], refs[n_o + n_w:n_o + 2 * n_w])
    y_ref, o_full = refs[-2:]
    n_cols = y_ref.shape[-1]
    head_dim = sides[0][0].shape[1]
    n_mates = n_o // n_tp

    @pl.when(pl.program_id(0) == 0)
    def _():
        for mate in range(n_mates):
            kv_idx = jnp.bitwise_xor(rank_ref[2], mate)
            for bit in range(n_tp):
                piece = o_refs[mate * n_tp + bit]
                source = jnp.bitwise_xor(rank_ref[0], bit)
                for head in range(heads):
                    part = jnp.bitwise_xor(rank_ref[1], kv_idx * heads + head)
                    col = pl.multiple_of((part * n_tp + source) * head_dim, head_dim)
                    o_full[:, pl.ds(col, head_dim)] = piece[:, head * head_dim:(head + 1) * head_dim]

    def columns(w_refs):
        total = None
        start = 0
        for w_ref in w_refs:
            depth = w_ref.shape[0] * head_dim
            term = jnp.dot(o_full[:, start:start + depth], w_ref[...].reshape(depth, n_cols), preferred_element_type=jnp.float32)
            total = term if total is None else total + term
            start += depth
        y_ref[...] = total.astype(y_ref.dtype)

    left = pl.program_id(0) < n_left
    pl.when(left)(functools.partial(columns, sides[0]))
    pl.when(jnp.logical_not(left))(functools.partial(columns, sides[1]))


def project(ranks, n_tp, pieces, w_sides, heads, n_cols=256):
    head_dim = w_sides[0][0].shape[1]
    rows, piece_cols = pieces[0].shape
    depth = sum(part.shape[0] for part in w_sides[0]) * head_dim
    n_left, n_right = [side[0].shape[2] // n_cols for side in w_sides]
    d_model = (n_left + n_right) * n_cols
    grid_spec = pltpu.PrefetchScalarGridSpec(
        num_scalar_prefetch=1,
        grid=(n_left + n_right,),
        in_specs=[pl.BlockSpec((rows, piece_cols), lambda i, t: (0, 0))] * len(pieces)
        + [pl.BlockSpec((part.shape[0], head_dim, n_cols), lambda i, t: (0, 0, jnp.minimum(i, n_left - 1))) for part in w_sides[0]]
        + [pl.BlockSpec((part.shape[0], head_dim, n_cols), lambda i, t: (0, 0, jnp.maximum(i - n_left, 0))) for part in w_sides[1]],
        out_specs=pl.BlockSpec((rows, n_cols), lambda i, t: (0, i)),
        scratch_shapes=[pltpu.VMEM((rows, depth), jnp.bfloat16)],
    )
    return pl.pallas_call(
        functools.partial(project_kernel, n_tp, heads, len(pieces), len(w_sides[0]), n_left),
        grid_spec=grid_spec,
        out_shape=jax.ShapeDtypeStruct((rows, d_model), jnp.bfloat16),
        compiler_params=pltpu.CompilerParams(dimension_semantics=("arbitrary",), vmem_limit_bytes=48 << 20),
        cost_estimate=pl.CostEstimate(flops=2 * rows * depth * d_model, bytes_accessed=40 << 20, transcendentals=0),
        name="project",
    )(ranks, *pieces, *w_sides[0], *w_sides[1])


def solution(mesh):
    n_cp = mesh.shape["cp"]
    n_tp = mesh.shape["tp"]
    n_dp = mesh.shape["dp"]

    def swap(arr, axis, bit):
        return lax.ppermute(arr, axis, [(src, src ^ bit) for src in range(mesh.shape[axis])])

    def send_rows(arr, mate, bit):
        perm = [(tp * n_cp + cp, (tp ^ bit) * n_cp + (cp ^ mate)) for tp in range(n_tp) for cp in range(n_cp)]
        return lax.ppermute(arr, ("tp", "cp"), perm) if mate or bit else arr

    calls = [(first_bit, mate) for first_bit in range(n_tp - 1, 0, -2) for mate in (1, 0)]

    def per_device(x_loc, seg_loc, w_q, w_k, w_v, w_o):
        cp_rank = lax.axis_index("cp")
        tp_rank = lax.axis_index("tp")
        own_rows, d_model = x_loc.shape
        kv_loc = w_k.shape[1]
        head_dim = w_k.shape[2]
        n_rows = own_rows * n_tp
        piece_len = n_rows // 2
        width = w_q.shape[1] * head_dim
        cuts = [0, own_rows * 3 // 4, own_rows]

        part_rows = w_o.shape[0] * head_dim // (n_dp * n_cp)
        part_idx = lax.axis_index("dp") * n_cp + cp_rank
        w_o_part = lax.dynamic_slice_in_dim(w_o.reshape(width, d_model), part_idx * part_rows, part_rows)
        col_cuts = [0, d_model // 4, d_model]
        mid_tp = n_tp // 2

        def gather_wo(side):
            w_tp = lax.all_gather(w_o_part[:, col_cuts[side]:col_cuts[side + 1]], "tp", axis=0)
            w_dp = swap(w_tp, "dp", 1)
            w_cp = swap(w_tp, "cp", 2)
            w_diag0 = swap(w_dp[:mid_tp], "cp", 2)
            w_diag1 = swap(w_cp[mid_tp:], "dp", 1)
            near = [w_tp, w_cp, w_dp, w_diag0, w_diag1]
            far = []
            for part in near:
                far.append(swap(part, "cp", 1))
            return [near[0], far[0], near[1], far[1], near[2], far[2], near[3], near[4], far[3], far[4]]

        x_parts = []
        for first, last in zip(cuts, cuts[1:]):
            x_parts.append(lax.all_gather(x_loc[first:last], "tp", axis=0, tiled=True))
        w_sides = [gather_wo(side) for side in range(2)]
        seg_all = lax.all_gather(seg_loc, ("cp", "tp"), axis=0, tiled=True)
        core = cp_rank % 2
        heads_per_kv = w_q.shape[1] // kv_loc
        w_q_heads = w_q.reshape(d_model, kv_loc, heads_per_kv * head_dim)
        w_q_keep, w_q_send = [lax.dynamic_index_in_dim(w_q_heads, core ^ mate, 1, False) for mate in range(2)]
        w_kv_keep, w_kv_send = [jnp.concatenate([lax.dynamic_index_in_dim(arr, core ^ mate, 1, False) for arr in (w_k, w_v)], axis=1) for mate in range(2)]

        tile_rows = own_rows // SUBS
        tile_row = jnp.arange(n_tp * SUBS) * tile_rows
        bounds, row_starts = [], []
        for mate in range(2):
            block = cp_rank ^ mate
            seg_rows = lax.dynamic_slice_in_dim(seg_all, block * n_rows, n_rows)
            row_start = jnp.sum((seg_all[None, :] < seg_rows[:, None]).astype(jnp.int32), axis=1)
            first_pos = jnp.where(tile_row < piece_len, block * piece_len + tile_row, (2 * n_cp - 1 - block) * piece_len + tile_row - piece_len)
            start_tiles = row_start.reshape(n_tp * SUBS, tile_rows)
            lo = start_tiles[:, 0] // own_rows
            full_end = first_pos // own_rows
            mid = jnp.minimum((start_tiles[:, -1] + own_rows - 1) // own_rows, full_end)
            bounds.append(jnp.stack([first_pos, lo, mid, full_end, full_end + 1, jnp.full_like(lo, cp_rank), jnp.full_like(lo, tp_rank)]).astype(jnp.int32))
            row_starts.append(row_start.reshape(-1, 1))
        x_parts[0], w_q_keep, w_q_send, w_kv_keep, w_kv_send, bounds, row_starts = lax.optimization_barrier((x_parts[0], w_q_keep, w_q_send, w_kv_keep, w_kv_send, bounds, row_starts))

        def rows_by(x_part, weights):
            return jnp.dot(x_part, weights, preferred_element_type=jnp.float32).astype(jnp.bfloat16)

        q_parts, kv_parts = [], []
        for x_part in x_parts:
            kv_send = rows_by(x_part, w_kv_send)
            kv_mate = swap(kv_send, "cp", 1)
            kv_keep = rows_by(x_part, w_kv_keep)
            kv_near = jnp.concatenate([kv_keep, kv_mate], axis=0)
            kv_far = swap(kv_near, "cp", 2)
            q_send = rows_by(x_part, w_q_send)
            q_mate = swap(q_send, "cp", 1)
            q_keep = rows_by(x_part, w_q_keep)
            q_parts.append((q_keep, q_mate))
            kv_parts.append(jnp.concatenate([kv_near, kv_far], axis=0))

        pieces = [None] * (2 * n_tp)
        for first_bit, mate in calls:
            tiles = flash(n_cp, n_tp, first_bit, [pair[mate] for pair in q_parts], kv_parts, head_dim, bounds[mate], row_starts[mate])
            for bit, mine in zip((first_bit, first_bit - 1), tiles):
                pieces[mate * n_tp + bit] = send_rows(mine, mate, bit)
        ranks = jnp.stack([tp_rank, part_idx, core]).astype(jnp.int32)
        return project(ranks, n_tp, pieces, w_sides, heads_per_kv)


    return jax.shard_map(
        per_device,
        mesh=mesh,
        in_specs=(P(("dp", "cp", "tp"), None), P(("dp", "cp", "tp")), P(None, "tp", None), P(None, "tp", None), P(None, "tp", None), P("tp", None, None)),
        out_specs=P(("dp", "cp", "tp"), None),
        check_vma=False,
    )
```
